128 devices in a mesh: half: 2 (over core), vocab: 32 (over y_hi, x, z), tok: 2 (over y_lo).
Axes of the slice: x: 4, y: 4 (y_hi: 2, y_lo: 2; y = y_hi * 2 + y_lo), z: 4, core: 2. Of those that a mesh axis runs over, the one named last changes fastest.
Arguments:
- teacher_hidden: bfloat16 [2048, 8192], P('vocab', ('half', 'tok')), may hold values from -400 to 400
- student_hidden: bfloat16 [2048, 4096], P('vocab', ('half', 'tok')), may hold values from -400 to 400
- teacher_gain: float32 [8192], P(('half', 'tok')), may hold values from 0.5 to 1.5
- student_gain: float32 [4096], P(('half', 'tok')), may hold values from 0.5 to 1.5
- teacher_head: bfloat16 [8192, 65536], P(('half', 'tok'), 'vocab'), may hold values from -1 to 1
- student_head: bfloat16 [4096, 65536], P(('half', 'tok'), 'vocab'), may hold values from -2 to 2
- labels: int32 [2048], P(('half', 'tok')), may hold values from 0 to 65535
Outputs:
- token_loss: float32 [2048], P(('half', 'tok'))
- logit_grad: bfloat16 [2048, 65536], P(('half', 'tok'), 'vocab')
The draws below stay inside these ranges and needn't reach their ends.
All inputs are finite; a program needn't handle non-finite values.
Results may differ from the reference program's by a relative error of at most 0.0068.
Values may be sent and summed in bfloat16 or wider, within the bound.
A program may use at most 192 MiB of HBM per device.

```python
import jax
import jax.numpy as jnp
from jax import lax

DT = 8192
DS = 4096
TOK = 2048
V = 65536


def hidden_rows(key, width):
    first, second, third = jax.random.split(key, 3)
    row_scale = jnp.exp(jax.random.uniform(first, (TOK, 1), minval=0.0, maxval=jnp.log(10.0)))
    ramp = jnp.exp(jnp.arange(width, dtype=jnp.float32) / width * jnp.log(3.0))
    col_scale = ramp[None, :] * jnp.exp(jax.random.uniform(second, (1, width), minval=-0.7, maxval=0.7))
    base = jnp.clip(jax.random.normal(third, (TOK, width)), -6.0, 6.0)
    return base * row_scale * col_scale


def drawn_head(key, width):
    weight_key = jax.random.fold_in(jax.random.fold_in(key, 7), 0)
    weight = jnp.clip(jax.random.normal(weight_key, (width, V)), -6.0, 6.0) * (4.0 / jnp.sqrt(jnp.float32(width)))
    return weight


def draw_teacher_hidden(key, part):
    return hidden_rows(jax.random.fold_in(key, 1), DT).astype(jnp.bfloat16)


def draw_student_hidden(key, part):
    return hidden_rows(jax.random.fold_in(key, 2), DS).astype(jnp.bfloat16)


def draw_teacher_head(key, part):
    return drawn_head(jax.random.fold_in(key, 1), DT).astype(jnp.bfloat16)


def draw_student_head(key, part):
    return drawn_head(jax.random.fold_in(key, 2), DS).astype(jnp.bfloat16)


def set_ends(entries, rng, low, high):
    index_at = [jax.random.randint(jax.random.fold_in(rng, axis), (), 0, length) for axis, length in enumerate(entries.shape)]
    widest = entries.shape.index(max(entries.shape))
    next_to = index_at[:widest] + [(index_at[widest] + 1) % entries.shape[widest]] + index_at[widest + 1:]
    return entries.at[tuple(index_at)].set(low).at[tuple(next_to)].set(high)


def setup_inputs(seed: int = 0) -> dict:
    seeds = jax.random.split(jax.random.key(seed), 8)
    teacher_hidden = draw_teacher_hidden(jax.random.fold_in(seeds[7], 71), 0)
    student_hidden = draw_student_hidden(jax.random.fold_in(seeds[7], 71), 0)
    teacher_gain = jnp.clip(1.0 + 0.1 * jax.random.normal(seeds[2], (DT,), jnp.float32), 0.5, 1.5)
    student_gain = jnp.clip(1.0 + 0.1 * jax.random.normal(seeds[3], (DS,), jnp.float32), 0.5, 1.5)
    teacher_head = draw_teacher_head(jax.random.fold_in(seeds[7], 71), 0)
    student_head = draw_student_head(jax.random.fold_in(seeds[7], 71), 0)
    labels = set_ends(jax.random.randint(seeds[6], (TOK,), 0, V), jax.random.fold_in(seeds[6], 1), 0, V - 1).astype(jnp.int32)
    return {"teacher_hidden": teacher_hidden, "student_hidden": student_hidden, "teacher_gain": teacher_gain, "student_gain": student_gain, "teacher_head": teacher_head, "student_head": student_head, "labels": labels}


epsilon = 1e-05
label_weight = 0.5

def head_logits(hidden, gain, head, width):
    values = hidden.astype(jnp.float32)
    squares = lax.optimization_barrier(jnp.sum(values * values, axis=1))
    scaled = (values * gain[None, :]).astype(jnp.bfloat16)
    inverse = lax.rsqrt(squares / width + epsilon)
    return jnp.dot(scaled, head, preferred_element_type=jnp.float32) * inverse[:, None]

def reference(teacher_hidden, student_hidden, teacher_gain, student_gain, teacher_head, student_head, labels):
    teacher_logits = head_logits(teacher_hidden, teacher_gain, teacher_head, DT)
    student_logits = head_logits(student_hidden, student_gain, student_head, DS)
    teacher_max = lax.optimization_barrier(jnp.max(teacher_logits, axis=1))
    student_max = lax.optimization_barrier(jnp.max(student_logits, axis=1))
    teacher_exp = jnp.exp(teacher_logits - teacher_max[:, None])
    student_exp = jnp.exp(student_logits - student_max[:, None])
    teacher_total = lax.optimization_barrier(jnp.sum(teacher_exp, axis=1))
    student_total = lax.optimization_barrier(jnp.sum(student_exp, axis=1))
    cross = lax.optimization_barrier(jnp.sum(teacher_exp * (teacher_logits - student_logits), axis=1))
    columns = lax.broadcasted_iota(jnp.int32, student_logits.shape, 1)
    is_label = columns == labels[:, None]
    target = lax.optimization_barrier(jnp.sum(jnp.where(is_label, student_logits, jnp.float32(0.0)), axis=1))
    student_lse = student_max + jnp.log(student_total)
    token_loss = cross / teacher_total - teacher_max - jnp.log(teacher_total) + student_lse + label_weight * (student_lse - target)
    teacher_prob = teacher_exp / teacher_total[:, None]
    student_prob = student_exp / student_total[:, None]
    logit_grad = (1.0 + label_weight) * student_prob - teacher_prob - label_weight * is_label.astype(jnp.float32)
    return (token_loss, logit_grad.astype(jnp.bfloat16))
```

```python
import jax
import jax.numpy as jnp
from jax import lax
from jax.experimental import pallas as pl
from jax.experimental.pallas import tpu as pltpu
from jax.sharding import PartitionSpec as P

DT = 8192
DS = 4096
EPS = 1e-05
LABEL_WEIGHT = 0.5

N = 4
ROWS = 64
MINE = 512
WIDE = 2048
COLS = 512
TILES = WIDE // COLS
PART = 64
FULL = 32000.0

f32 = jnp.float32
bf16 = jnp.bfloat16
i16 = jnp.int16
MESH = pl.DeviceIdType.MESH


def remote(src, dst, send, recv, where):
    return pltpu.make_async_remote_copy(
        src_ref=src, dst_ref=dst, send_sem=send, recv_sem=recv, device_id=where, device_id_type=MESH
    )


def turned(row):
    return jnp.transpose(jnp.concatenate([row] * 16, axis=0))


def joined(a, b):
    t_max = jnp.maximum(a[0:1], b[0:1])
    t_a, t_b = jnp.exp(a[0:1] - t_max), jnp.exp(b[0:1] - t_max)
    s_max = jnp.maximum(a[3:4], b[3:4])
    s_a, s_b = jnp.exp(a[3:4] - s_max), jnp.exp(b[3:4] - s_max)
    return jnp.concatenate(
        [
            t_max,
            a[1:2] * t_a + b[1:2] * t_b,
            a[2:3] * t_a + b[2:3] * t_b,
            s_max,
            a[4:5] * s_a + b[4:5] * s_b,
            a[5:6] + b[5:6],
            a[6:8],
        ],
        axis=0,
    )


def kernel(
    th, sh, gt, gs, lab, wt, ws, loss, grad,
    XS, XT, WS, WT, GS, GT, QS, SQ, INV, NS, NT, ACC, OS, OT, US, UT, RS, RT, OUT,
    MS, LS, TG, MT, LT, CR, STA, STR, FIN,
    x0_send, x0_recv, q_send, q_recv, i_send, i_recv, w_send, w_recv, w_loc,
    r_send, r_recv, e_send, e_recv, s_send, s_recv, o_sem,
):
    h, v, t = lax.axis_index("half"), lax.axis_index("vocab"), lax.axis_index("tok")
    yh = v // 16
    x = (v % 16) // 4
    z = v % 4
    far = (v + 16) % 32
    started = []

    def go(copy):
        copy.start()
        started.append(copy)

    def at(xx, zz):
        return {"half": h, "vocab": yh * 16 + (xx % N) * N + zz % N, "tok": t}

    values_t = th[...].astype(f32)
    values_s = sh[...].astype(f32)
    GT[...] = (values_t * gt[...]).astype(bf16)
    GS[...] = (values_s * gs[...]).astype(bf16)
    squares = jnp.concatenate(
        [
            jnp.sum(values_t * values_t, axis=1, keepdims=True),
            jnp.sum(values_s * values_s, axis=1, keepdims=True),
        ],
        axis=0,
    )
    q = h * 2 + t
    QS[...] = jnp.transpose(jnp.broadcast_to(squares, (128, 128)))[0:8]

    @pl.when(h == yh)
    def _():
        SQ[q] = QS[...]
        XS[h, x, z] = GS[...]
        XT[h, x, z] = GT[...]

    barrier = pltpu.get_barrier_semaphore()
    near = [
        {"half": (h + a) % 2, "vocab": (v + 16 * b) % 32, "tok": (t + c) % 2}
        for a in (0, 1) for b in (0, 1) for c in (0, 1) if a + b + c
    ]
    near += [at(x, z + d) for d in (1, 2, 3)] + [at(x + d, z) for d in (1, 2, 3)]
    for where in near:
        pl.semaphore_signal(barrier, inc=1, device_id=where, device_id_type=MESH)
    pl.semaphore_wait(barrier, len(near))

    sets = ((GS, XS, 0), (GT, XT, 1))

    def first(k, where_far):
        g, X, _ = sets[k]
        return remote(
            g, X.at[h, x, z], x0_send.at[k, int(where_far)], x0_recv.at[k, h],
            {"half": yh, "vocab": far if where_far else v, "tok": t},
        )

    def squares_to(b, c):
        return remote(
            QS, SQ.at[q], q_send.at[2 * b + c], q_recv.at[q],
            {"half": yh, "vocab": (v + 16 * b) % 32, "tok": (t + c) % 2},
        )

    def first_arrived(k, c):
        X = sets[k][1]
        remote(X.at[c, x, z], X.at[c, x, z], x0_send.at[k, 0], x0_recv.at[k, c], near[0]).wait_recv()

    go(first(0, True))

    @pl.when(h != yh)
    def _():
        first(0, False).start()
        squares_to(0, 0).start()
        first(1, False).start()

    for b, c in ((0, 1), (1, 0), (1, 1)):
        go(squares_to(b, c))
    go(first(1, True))

    other = near[3]
    loads = [
        pltpu.make_async_copy(ws, WS.at[h], w_loc.at[0]),
        pltpu.make_async_copy(wt, WT.at[h], w_loc.at[1]),
    ]
    for k, (w, W) in enumerate(((ws, WS), (wt, WT))):
        go(remote(w, W.at[h], w_send.at[k], w_recv.at[k], other))
        loads[k].start()

    def head_here(k):
        W = (WS, WT)[k]
        loads[k].wait()
        remote(W.at[1 - h], W.at[1 - h], w_send.at[k], w_recv.at[k], other).wait_recv()

    def steps(k, c):
        X = sets[k][1]
        half_rows = ROWS // 2

        def block(r, lo=None):
            xx, zz = (x, r % N) if c == 0 else (r % N, z)
            return X.at[c, xx, zz] if lo is None else X.at[c, xx, zz, pl.ds(lo, half_rows)]

        def line(r, lo=None):
            if c == 0:
                return X.at[0, r % N] if lo is None else X.at[0, r % N, pl.ds(lo, 2)]
            return X.at[1, :, r % N] if lo is None else X.at[1, pl.ds(lo, 2), r % N]

        a, b = (z, x) if c == 0 else (x, z)

        def to(phase, d):
            along_z = (phase == 0) == (c == 0)
            return at(x, z + d) if along_z else at(x + d, z)

        def copy(step, ref, where):
            return remote(ref, ref, r_send.at[k, c, step], r_recv.at[k, c, step], where)

        sends = (
            (copy(0, block(a), to(0, 1)), copy(1, block(a), to(0, 3))),
            (copy(2, block(a + 3, 0), to(0, 1)), copy(3, block(a + 1, half_rows), to(0, 3))),
            (copy(4, line(b), to(1, 1)), copy(5, line(b), to(1, 3))),
            (copy(6, line(b + 3, 0), to(1, 1)), copy(7, line(b + 1, 2), to(1, 3))),
        )
        takes = (
            (copy(0, block(a + 3), to(0, 3)), copy(1, block(a + 1), to(0, 1))),
            (copy(2, block(a + 2, 0), to(0, 3)), copy(3, block(a + 2, half_rows), to(0, 1))),
            (copy(4, line(b + 3), to(1, 3)), copy(5, line(b + 1), to(1, 1))),
            (copy(6, line(b + 2, 0), to(1, 3)), copy(7, line(b + 2, 2), to(1, 1))),
        )
        return sends, takes

    plans = [[steps(k, c) for c in (0, 1)] for k in (0, 1)]

    def send(k, step):
        for c in (0, 1):
            for copy in plans[k][c][0][step]:
                go(copy)

    def take(k, step):
        for c in (0, 1):
            for copy in plans[k][c][1][step]:
                copy.wait_recv()

    def first_take(k):
        first_arrived_mine = 1 - h

        @pl.when(h == yh)
        def _():
            first_arrived(k, first_arrived_mine)

        @pl.when(h != yh)
        def _():
            first_arrived(k, 0)
            first_arrived(k, 1)

    first_take(0)
    send(0, 0)

    for j in range(4):
        def arrived(j=j):
            remote(SQ.at[j], SQ.at[j], q_send.at[0], q_recv.at[j], near[0]).wait_recv()

        pl.when(jnp.logical_or(h != yh, q != j))(arrived)
    lane = lax.broadcasted_iota(jnp.int32, (8, 128), 1)
    total = (SQ[0] + SQ[1]) + (SQ[2] + SQ[3])
    INV[x, z] = lax.rsqrt(jnp.where(lane < 64, total / DT, total / DS) + EPS)

    take(0, 0)
    send(0, 1)
    for d in (1, 2, 3):
        go(remote(INV.at[x, z], INV.at[x, z], i_send.at[0, d - 1], i_recv.at[0, d - 1], at(x, z + d)))
    first_take(1)
    send(1, 0)
    take(0, 1)
    send(0, 2)
    for d in (1, 2, 3):
        ref = INV.at[x, (z + N - d) % N]
        remote(ref, ref, i_send.at[0, d - 1], i_recv.at[0, d - 1], at(x, z + N - d)).wait_recv()
    for d in (1, 2, 3):
        go(remote(INV.at[x], INV.at[x], i_send.at[1, d - 1], i_recv.at[1, d - 1], at(x + d, z)))
    take(0, 2)
    send(0, 3)
    take(1, 0)
    send(1, 1)
    for d in (1, 2, 3):
        ref = INV.at[(x + N - d) % N]
        remote(ref, ref, i_send.at[1, d - 1], i_recv.at[1, d - 1], at(x + N - d, z)).wait_recv()
    spread = jnp.transpose(INV[...].reshape(128, 128))
    for j in range(16):
        NT[j // 4, j % 4] = jnp.broadcast_to(spread[0:64, 8 * j : 8 * j + 1], (64, 128))
        NS[j // 4, j % 4] = jnp.broadcast_to(spread[64:128, 8 * j : 8 * j + 1], (64, 128))
    head_here(0)
    take(0, 3)
    take(1, 1)
    send(1, 2)

    theirs, ours = 2 * (1 - t), 2 * t
    across = {"half": h, "vocab": v, "tok": 1 - t}

    def product(k, x0, n):
        X, W = sets[k][1], (WS, WT)[k]
        cols = pl.ds(pl.multiple_of(n * COLS, COLS), COLS)
        width = X.shape[-1]
        parts = [
            jnp.dot(X[c, pl.ds(x0, 2)].reshape(MINE, width), W[c, :, cols], preferred_element_type=f32)
            for c in (0, 1)
        ]
        return parts[0] + parts[1]

    def exchange(k, n):
        U, R = ((US, RS), (UT, RT))[k]
        return remote(U.at[n], R.at[n], e_send.at[k, n], e_recv.at[k, n], across)

    def theirs_tile(k, n):
        U, inv = (US, UT)[k], (NS, NT)[k]
        ACC[...] = product(k, theirs, n)

        def part(j, bounds):
            rows = pl.ds(pl.multiple_of(j * PART, PART), PART)
            value = ACC[rows, :] * jnp.concatenate([inv[theirs + j // 4, j % 4]] * (COLS // 128), axis=1)
            ACC[rows, :] = value
            size = jnp.max(jnp.abs(value), axis=1, keepdims=True)
            power = jnp.ceil(jnp.log2(jnp.maximum(size, 1e-30)) + 1e-4)
            STA[rows, :] = jnp.broadcast_to(power, (PART, 128))
            U[n, rows, :] = jnp.round(value * (jnp.exp2(-power) * FULL)).astype(jnp.int32).astype(i16)
            return bounds

        lax.fori_loop(0, MINE // PART, part, 0)
        U[n, pl.ds(MINE, 16), :] = jnp.transpose(STA[...])[0:16].astype(jnp.int32).astype(i16)

    def theirs_tiles(k):
        def tile(n, carry):
            theirs_tile(k, n)

            @pl.when(n > 0)
            def _():
                exchange(k, n - 1).start()

            return carry

        lax.fori_loop(0, TILES, tile, 0)

    def ours_tiles(k):
        O = (OS, OT)[k]

        def tile(n, carry):
            O[n] = product(k, ours, n)

            @pl.when(n == 0)
            def _():
                exchange(k, TILES - 1).start()

            return carry

        lax.fori_loop(0, TILES, tile, 0)

    theirs_tiles(0)
    ours_tiles(0)
    take(1, 2)
    send(1, 3)
    head_here(1)
    take(1, 3)
    theirs_tiles(1)
    ours_tiles(1)

    label = turned(jnp.broadcast_to(lab[...].astype(f32), (8, MINE))).astype(jnp.int32)
    FIN[...] = label.astype(f32)
    low = jnp.full((MINE, 128), -3.0e38, f32)
    none = jnp.zeros((MINE, 128), f32)
    MS[...] = low
    MT[...] = low
    for ref in (LS, TG, LT, CR):
        ref[...] = none

    def arrive(k, n):
        O, R, inv, M, L = ((OS, RS, NS, MS, LS), (OT, RT, NT, MT, LT))[k]
        exchange(k, n).wait_recv()
        head = R[n, pl.ds(MINE, 16), :].astype(jnp.int32).astype(f32)[0:8]
        STA[...] = turned(head)

        def part(j, carry):
            rows = pl.ds(pl.multiple_of(j * PART, PART), PART)
            scale = jnp.exp2(STA[rows, :]) * (1.0 / FULL)
            norm = inv[ours + j // 4, j % 4]
            groups = []
            for g in range(COLS // 128):
                cols = pl.ds(g * 128, 128)
                sent = R[n, rows, cols].astype(jnp.int32).astype(f32)
                groups.append(O[n, rows, cols] * norm + sent * scale)
                O[n, rows, cols] = groups[g]
            old = M[rows, :]
            new = old
            for value in groups:
                new = jnp.maximum(new, value)
            shrink = jnp.exp(old - new)
            sums = L[rows, :] * shrink
            if k == 1:
                cross = CR[rows, :] * shrink
            else:
                target = TG[rows, :]
                label = FIN[rows, :].astype(jnp.int32)
                base = v * WIDE + n * COLS + lax.broadcasted_iota(jnp.int32, (PART, 128), 1)
            for g, value in enumerate(groups):
                grown = jnp.exp(value - new)
                sums = sums + grown
                if k == 1:
                    cross = cross + grown * (value - OS[n, rows, pl.ds(g * 128, 128)])
                else:
                    target = target + jnp.where(base + g * 128 == label, value, 0.0)
            M[rows, :] = new
            L[rows, :] = sums
            if k == 1:
                CR[rows, :] = cross
            else:
                TG[rows, :] = target
            return carry

        lax.fori_loop(0, MINE // PART, part, 0)

    for k in (0, 1):
        def arrived_tile(n, carry, k=k):
            arrive(k, n)
            return carry

        lax.fori_loop(0, TILES, arrived_tile, 0)

    def lanes(j, carry):
        rows = pl.ds(pl.multiple_of(j * PART, PART), PART)
        m_t, m_s = MT[rows, :], MS[rows, :]
        t_max = jnp.max(m_t, axis=1, keepdims=True)
        s_max = jnp.max(m_s, axis=1, keepdims=True)
        w_t, w_s = jnp.exp(m_t - t_max), jnp.exp(m_s - s_max)
        columns = (
            t_max,
            jnp.sum(LT[rows, :] * w_t, axis=1, keepdims=True),
            jnp.sum(CR[rows, :] * w_t, axis=1, keepdims=True),
            s_max,
            jnp.sum(LS[rows, :] * w_s, axis=1, keepdims=True),
            jnp.sum(TG[rows, :], axis=1, keepdims=True),
        )
        lane = lax.broadcasted_iota(jnp.int32, (PART, 128), 1)
        packed = jnp.zeros((PART, 128), f32)
        for i, column in enumerate(columns):
            packed = jnp.where(lane == i, column, packed)
        STA[rows, :] = packed
        return carry

    lax.fori_loop(0, MINE // PART, lanes, 0)
    STR[0] = jnp.transpose(STA[...])[0:8]

    def meet(base, offsets, places, me, count):
        for i, where in enumerate(places):
            go(remote(STR.at[base], STR.at[base + 1 + i], s_send.at[base + i], s_recv.at[base + i], where))
        for i, where in enumerate(places):
            ref = STR.at[base + 1 + i]
            remote(ref, ref, s_send.at[base + i], s_recv.at[base + i], where).wait_recv()
        out = STR[base]
        for i in range(len(places)):
            out = joined(out, STR[base + 1 + i])
        return out

    STR[4] = meet(0, None, [at(x, z + d) for d in (1, 2, 3)], z, N)
    STR[8] = meet(4, None, [at(x + d, z) for d in (1, 2, 3)], x, N)
    whole = meet(8, None, [{"half": h, "vocab": far, "tok": t}], yh, 2)

    t_max, t_total, cross = whole[0:1], whole[1:2], whole[2:3]
    s_max, s_total, target = whole[3:4], whole[4:5], whole[5:6]
    student_lse = s_max + jnp.log(s_total)
    loss[...] = (
        cross / t_total - t_max - jnp.log(t_total) + student_lse + LABEL_WEIGHT * (student_lse - target)
    )
    factors = jnp.concatenate(
        [s_max, (1.0 + LABEL_WEIGHT) / s_total, t_max, 1.0 / t_total, jnp.zeros((124, MINE), f32)],
        axis=0,
    )
    STA[...] = jnp.transpose(factors)

    def results(j, carry):
        rows = pl.ds(pl.multiple_of(j * PART, PART), PART)
        per_row = STA[rows, :]
        m_s, c_s, m_t, c_t = (jnp.broadcast_to(per_row[:, i : i + 1], (PART, 128)) for i in range(4))
        label = FIN[rows, :].astype(jnp.int32)
        column = v * WIDE + lax.broadcasted_iota(jnp.int32, (PART, 128), 1)
        for n in range(TILES):
            for g in range(COLS // 128):
                cols = pl.ds(g * 128, 128)
                value = jnp.exp(OS[n, rows, cols] - m_s) * c_s - jnp.exp(OT[n, rows, cols] - m_t) * c_t
                here = column + (n * COLS + g * 128) == label
                value = value - jnp.where(here, LABEL_WEIGHT, 0.0)
                OUT[rows, pl.ds(n * COLS + g * 128, 128)] = value.astype(bf16)
        return carry

    lax.fori_loop(0, MINE // PART, results, 0)
    out = pltpu.make_async_copy(OUT, grad, o_sem)
    out.start()

    for copy in started:
        copy.wait_send()

    @pl.when(h != yh)
    def _():
        first(0, False).wait_send()
        squares_to(0, 0).wait_send()
        first(1, False).wait_send()

    for k in (0, 1):
        for n in range(TILES):
            exchange(k, n).wait_send()
    out.wait()


def shards(th, sh, gt, gs, wt, ws, labels):
    kt, ks = wt.shape[0], ws.shape[0]
    vmem = pl.BlockSpec(memory_space=pltpu.VMEM)
    hbm = pl.BlockSpec(memory_space=pl.ANY)
    dma = pltpu.SemaphoreType.DMA
    V = pltpu.VMEM
    scratch = [
        V((2, N, N, ROWS, ks), bf16), V((2, N, N, ROWS, kt), bf16),
        V((2, ks, WIDE), bf16), V((2, kt, WIDE), bf16),
        V((ROWS, ks), bf16), V((ROWS, kt), bf16),
        V((8, 128), f32), V((4, 8, 128), f32), V((N, N, 8, 128), f32),
        V((N, N, ROWS, 128), f32), V((N, N, ROWS, 128), f32),
        V((MINE, COLS), f32),
        V((TILES, MINE, COLS), f32), V((TILES, MINE, COLS), f32),
        V((TILES, MINE + 16, COLS), i16), V((TILES, MINE + 16, COLS), i16),
        V((TILES, MINE + 16, COLS), i16), V((TILES, MINE + 16, COLS), i16),
        V((MINE, WIDE), bf16),
        *[V((MINE, 128), f32) for _ in range(7)],
        V((10, 8, MINE), f32),
        V((MINE, 128), f32),
        dma((2, 2)), dma((2, 2)), dma((4,)), dma((4,)), dma((2, 3)), dma((2, 3)),
        dma((2,)), dma((2,)), dma((2,)),
        dma((2, 2, 8)), dma((2, 2, 8)), dma((2, TILES)), dma((2, TILES)), dma((10,)), dma((10,)),
        dma,
    ]
    loss, grad = pl.pallas_call(
        kernel,
        out_shape=(
            jax.ShapeDtypeStruct((1, MINE), f32),
            jax.ShapeDtypeStruct((MINE, WIDE), bf16),
        ),
        in_specs=[vmem] * 5 + [hbm] * 2,
        out_specs=(vmem, hbm),
        scratch_shapes=scratch,
        compiler_params=pltpu.CompilerParams(
            collective_id=0, has_side_effects=True, vmem_limit_bytes=67043328
        ),
    )(th, sh, gt.reshape(1, kt), gs.reshape(1, ks), labels.reshape(1, MINE), wt, ws)
    return loss.reshape(MINE), grad


def solution(mesh):
    return jax.shard_map(
        shards,
        mesh=mesh,
        in_specs=(
            P("vocab", ("half", "tok")),
            P("vocab", ("half", "tok")),
            P(("half", "tok")),
            P(("half", "tok")),
            P(("half", "tok"), "vocab"),
            P(("half", "tok"), "vocab"),
            P(("half", "tok")),
        ),
        out_specs=(P(("half", "tok")), P(("half", "tok"), "vocab")),
        check_vma=False,
    )
```
